32 devices in a mesh: row: 8 (over y, x, core), col: 4 (over z).
Axes of the slice: x: 2, y: 2, z: 4, core: 2. Of those that a mesh axis runs over, the one named last changes fastest.
Arguments:
- value_proj: float32 [8, 4, 1024, 512], P('row', 'col'), may hold values from -6 to 6
- token_pool: bfloat16 [8, 4, 1536, 1024], P('row', 'col'), may hold values from -6 to 6
- target_pool: bfloat16 [8, 4, 1536, 1024], P('row', 'col'), may hold values from -6 to 6
- batch_ids: int32 [8, 4, 3, 1536], P('row', 'col'), may hold values from 0 to 1535
- frozen_out: bfloat16 [512, 1024], replicated, may hold values from -0.25 to 0.25
- numerators: int32 [3], replicated, may hold values from 4 to 15
Outputs:
- final_proj: float32 [8, 4, 1024, 512], P('row', 'col')
- final_tracker: float32 [8, 4, 1024, 512], P('row', 'col')
The draws below stay inside these ranges and needn't reach their ends.
All inputs are finite; a program needn't handle non-finite values.
Results may differ from the reference program's by a relative error of at most 0.017.
Values sent between devices are 32-bit elements; how exact they have to be, the bound alone decides.
No kernel may reach another device: no remote copies, remote signals or barrier semaphores. Data moves between devices by JAX's collectives and lax.ppermute only.
A program may use at most 128 MiB of HBM per device.

```python
import jax
import jax.numpy as jnp
from jax import lax

D = 1024
HD = 512
BATCH = 1536
ITERS = 2
POOL = 1536
N_ROW = 8
N_COL = 4


def plant(drawn, stream_key, low, high):
    longest = drawn.shape.index(max(drawn.shape))
    spots = []
    for shift in (0, 1):
        where = [jax.random.randint(jax.random.fold_in(stream_key, axis), (), 0, length) for axis, length in enumerate(drawn.shape)]
        where[longest] = (where[longest] + shift) % drawn.shape[longest]
        spots.append(tuple(where))
    return drawn.at[spots[0]].set(low).at[spots[1]].set(high)


def steps_of(stream_key, shape, split, least, top_value):
    level, own = 1.0, jax.random.fold_in(stream_key, 6)
    for dim, parts in split:
        draws = jnp.exp(jax.random.uniform(jax.random.fold_in(own, dim), (parts,), jnp.float32, least / len(split), top_value / len(split)))
        level = level * jnp.repeat(draws, shape[dim] // parts).reshape([-1 if axis == dim else 1 for axis in range(len(shape))])
    return level


def normal_values(key, dims, width, reach, pieces=(), held_as=jnp.bfloat16):
    values = width * jax.random.normal(key, dims, jnp.float32)
    if pieces:
        values = values * steps_of(key, dims, pieces, -0.22, 0.18)
    return jnp.clip(values, -reach, reach).astype(held_as)


def setup_inputs(seed: int = 0) -> dict:
    streams_of = jax.random.split(jax.random.key(seed), 7)
    return {
        "value_proj": normal_values(streams_of[0], (N_ROW, N_COL, D, HD), 1.0, 6.0, ((0, 8), (1, 4)), jnp.float32),
        "token_pool": normal_values(streams_of[1], (N_ROW, N_COL, POOL, D), 1.0, 6.0, ((0, 8), (1, 4))),
        "target_pool": normal_values(streams_of[2], (N_ROW, N_COL, POOL, D), 1.0, 6.0, ((0, 8), (1, 4))),
        "batch_ids": plant(jax.random.randint(streams_of[3], (N_ROW, N_COL, ITERS + 1, BATCH), 0, POOL), jax.random.fold_in(streams_of[3], 1), 0, POOL - 1).astype(jnp.int32),
        "frozen_out": normal_values(streams_of[4], (HD, D), HD ** -0.5, 0.25),
        "numerators": jax.random.randint(streams_of[5], (3,), 4, 16).astype(jnp.int32),
    }


step_rate = 0.2


def grad_single(current, pool_rows, target_rows, chosen, frozen_out):
    factor = D ** -0.5
    tokens = pool_rows[chosen]
    targets = target_rows[chosen]
    preact = jnp.dot(tokens, current.astype(jnp.bfloat16), preferred_element_type=jnp.float32) * factor
    sigmoid_pre = jax.nn.sigmoid(preact)
    hidden = (preact * sigmoid_pre).astype(jnp.bfloat16)
    output = jnp.dot(hidden, frozen_out, preferred_element_type=jnp.float32)
    error_term = (output - targets.astype(jnp.float32)).astype(jnp.bfloat16)
    back_hidden = lax.dot_general(error_term, frozen_out, (((1,), (1,)), ((), ())), preferred_element_type=jnp.float32)
    slope = sigmoid_pre * (1.0 + preact * (1.0 - sigmoid_pre))
    back_pre = (back_hidden * slope).astype(jnp.bfloat16)
    return lax.dot_general(tokens, back_pre, (((0,), (0,)), ((), ())), preferred_element_type=jnp.float32) * factor


def all_gradients(current, token_pool, target_pool, batch_ids, frozen_out, which):
    count = N_ROW * N_COL

    def flatten(array):
        return array.reshape((count,) + array.shape[2:])

    def single(items):
        return grad_single(items[0], items[1], items[2], items[3], frozen_out)

    result = lax.map(single, (flatten(current), flatten(token_pool), flatten(target_pool), flatten(batch_ids[:, :, which])))
    return result.reshape(current.shape)


def gossip(field, mix_weights):
    return mix_weights[0] * field + mix_weights[1] * jnp.roll(field, 1, 0) + mix_weights[2] * jnp.roll(field, 1, 1)


def reference(value_proj, token_pool, target_pool, batch_ids, frozen_out, numerators):
    counts = numerators.astype(jnp.float32)
    mix_weights = counts / jnp.sum(counts)
    current = value_proj
    grad_old = all_gradients(current, token_pool, target_pool, batch_ids, frozen_out, 0)
    tracker = grad_old
    for which in range(1, ITERS + 1):
        current_new = gossip(current, mix_weights) - step_rate * tracker
        grad_new = all_gradients(current_new, token_pool, target_pool, batch_ids, frozen_out, which)
        tracker = (gossip(tracker, mix_weights) + grad_new) - grad_old
        current = current_new
        grad_old = grad_new
    return current, tracker
```

```python
import functools

import jax
import jax.numpy as jnp
from jax import lax
from jax.experimental import pallas as pl
from jax.experimental.pallas import tpu as pltpu
from jax.sharding import PartitionSpec as P

ITERS = 2

step_rate = 0.2


def shifted(block, axis, distance):
    devices = range(lax.axis_size(axis))
    route = [((i - distance) % len(devices), i) for i in devices]
    return lax.ppermute(block, axis, route)


def tile_of(rows, most):
    tile = min(rows, most)
    while rows % tile:
        tile -= 8
    return tile


def gradient_body(which, tile, factor, ids_ref, x_ref, tok_ref, tgt_ref, out_ref, g_ref, xb_ref):
    step = pl.program_id(0)

    @pl.when(step == 0)
    def _():
        xb_ref[...] = x_ref[...].astype(jnp.bfloat16)

    tokens = tok_ref[...]
    frozen = out_ref[...]
    preact = jnp.dot(tokens, xb_ref[...], preferred_element_type=jnp.float32) * factor
    sigmoid_pre = jax.nn.sigmoid(preact)
    hidden = (preact * sigmoid_pre).astype(jnp.bfloat16)
    output = jnp.dot(hidden, frozen, preferred_element_type=jnp.float32)
    error_term = (output - tgt_ref[...].astype(jnp.float32)).astype(jnp.bfloat16)
    back_hidden = lax.dot_general(
        error_term, frozen, (((1,), (1,)), ((), ())), preferred_element_type=jnp.float32
    )
    slope = sigmoid_pre * (1.0 + preact * (1.0 - sigmoid_pre))
    rows = lax.broadcasted_iota(jnp.int32, (tile, ids_ref.shape[1]), 0) + step * tile
    named = jnp.where(rows == ids_ref[which : which + 1, :], 1.0, 0.0)
    times = jnp.sum(named, axis=1, keepdims=True)
    back_pre = (back_hidden * slope * times).astype(jnp.bfloat16)
    part = factor * lax.dot_general(
        tokens, back_pre, (((0,), (0,)), ((), ())), preferred_element_type=jnp.float32
    )

    @pl.when(step == 0)
    def _():
        g_ref[...] = part

    @pl.when(step > 0)
    def _():
        g_ref[...] += part


def local_gradient(which, current, tokens, targets, ids, frozen_out):
    pool, width = tokens.shape
    heads = current.shape[1]
    tile = tile_of(pool, 512)
    whole = lambda shape: pl.BlockSpec(shape, lambda i: (0, 0))
    return pl.pallas_call(
        functools.partial(gradient_body, which, tile, width ** (-0.5)),
        grid=(pool // tile,),
        in_specs=[
            whole(ids.shape),
            whole(current.shape),
            pl.BlockSpec((tile, width), lambda i: (i, 0)),
            pl.BlockSpec((tile, width), lambda i: (i, 0)),
            whole(frozen_out.shape),
        ],
        out_specs=whole((width, heads)),
        out_shape=jax.ShapeDtypeStruct((width, heads), jnp.float32),
        scratch_shapes=[pltpu.VMEM(current.shape, jnp.bfloat16)],
        compiler_params=pltpu.CompilerParams(
            dimension_semantics=("arbitrary",), vmem_limit_bytes=32 * 2**20
        ),
        cost_estimate=pl.CostEstimate(
            flops=8 * pool * width * heads, bytes_accessed=12 * 2**20, transcendentals=0
        ),
        name=f"gradient_{which}",
    )(ids, current, tokens, targets, frozen_out)


def add_body(weight_ref, rest_ref, piece_ref, out_ref):
    out_ref[...] = rest_ref[...] + weight_ref[0] * piece_ref[...]


def add_piece(weight, rest, piece, start):
    rows, heads = piece.shape
    tile = tile_of(rows, 128)
    first = start // tile
    return pl.pallas_call(
        add_body,
        grid=(rows // tile,),
        in_specs=[
            pl.BlockSpec(memory_space=pltpu.SMEM),
            pl.BlockSpec((tile, heads), lambda i: (i + first, 0)),
            pl.BlockSpec((tile, heads), lambda i: (i, 0)),
        ],
        out_specs=pl.BlockSpec((tile, heads), lambda i: (i + first, 0)),
        out_shape=jax.ShapeDtypeStruct(rest.shape, rest.dtype),
        input_output_aliases={1: 0},
        compiler_params=pltpu.CompilerParams(vmem_limit_bytes=4 * 2**20),
        cost_estimate=pl.CostEstimate(
            flops=2 * rows * heads, bytes_accessed=12 * rows * heads, transcendentals=0
        ),
        name="add_piece",
    )(weight, rest, piece)


def combine(mix_weights, own, from_row, from_col):
    return mix_weights[0] * own + mix_weights[1] * from_row + mix_weights[2] * from_col


def on_device(value_proj, token_pool, target_pool, batch_ids, frozen_out, numerators):
    counts = numerators.astype(jnp.float32)
    mix_weights = counts / jnp.sum(counts)
    current = value_proj[0, 0]

    def gradient_at(field, which):
        return local_gradient(
            which, field, token_pool[0, 0], target_pool[0, 0], batch_ids[0, 0], frozen_out
        )

    def neighbours(field):
        from_col = shifted(field, "col", 1)
        return shifted(field, "row", 1), from_col

    around_current = neighbours(current)
    grad_old = gradient_at(current, 0)
    tracker = grad_old
    for which in range(1, ITERS):
        around_tracker = neighbours(tracker)
        current = combine(mix_weights, current, *around_current) - step_rate * tracker
        around_current = neighbours(current)
        grad_new = gradient_at(current, which)
        tracker = combine(mix_weights, tracker, *around_tracker) + grad_new - grad_old
        tracker = lax.optimization_barrier(tracker)
        grad_old = grad_new

    width = tracker.shape[0]
    cuts = [0, width * 3 // 4, width]
    pieces = [shifted(tracker[a:b], "col", 1) for a, b in zip(cuts, cuts[1:])]
    track_row = shifted(tracker, "row", 1)
    current = combine(mix_weights, current, *around_current) - step_rate * tracker
    grad_new = gradient_at(current, ITERS)
    rest = mix_weights[0] * tracker + mix_weights[1] * track_row + (grad_new - grad_old)
    for start, piece in zip(cuts, pieces):
        rest = add_piece(mix_weights[2:], rest, piece, start)
    return (current[None, None], rest[None, None])


def solution(mesh):
    return jax.shard_map(
        on_device,
        mesh=mesh,
        in_specs=(
            P("row", "col", None, None),
            P("row", "col", None, None),
            P("row", "col", None, None),
            P("row", "col", None, None),
            P(),
            P(),
        ),
        out_specs=(P("row", "col", None, None), P("row", "col", None, None)),
        check_vma=False,
    )
```

```python
import functools

import jax
import jax.numpy as jnp
from jax import lax
from jax.experimental import pallas as pl
from jax.experimental.pallas import tpu as pltpu
from jax.sharding import PartitionSpec as P


ITERS = 2

step_rate = 0.2


def shifted(block, axis, distance):
    devices = range(lax.axis_size(axis))
    route = [((i - distance) % len(devices), i) for i in devices]
    return lax.ppermute(block, axis, route)


def tile_of(rows, most):
    tile = min(rows, most)
    while rows % tile:
        tile -= 8
    return tile


def gradient_body(which, tile, factor, ids_ref, x_ref, tok_ref, tgt_ref, out_ref, g_ref, xb_ref):
    step = pl.program_id(0)

    @pl.when(step == 0)
    def _():
        xb_ref[...] = x_ref[...].astype(jnp.bfloat16)

    tokens = tok_ref[...]
    frozen = out_ref[...]
    preact = jnp.dot(tokens, xb_ref[...], preferred_element_type=jnp.float32) * factor
    sigmoid_pre = jax.nn.sigmoid(preact)
    hidden = (preact * sigmoid_pre).astype(jnp.bfloat16)
    output = jnp.dot(hidden, frozen, preferred_element_type=jnp.float32)
    error_term = (output - tgt_ref[...].astype(jnp.float32)).astype(jnp.bfloat16)
    back_hidden = lax.dot_general(
        error_term, frozen, (((1,), (1,)), ((), ())), preferred_element_type=jnp.float32
    )
    slope = sigmoid_pre * (1.0 + preact * (1.0 - sigmoid_pre))
    rows = lax.broadcasted_iota(jnp.int32, (tile, ids_ref.shape[1]), 0) + step * tile
    named = jnp.where(rows == ids_ref[which : which + 1, :], 1.0, 0.0)
    times = jnp.sum(named, axis=1, keepdims=True)
    back_pre = (back_hidden * slope * times).astype(jnp.bfloat16)
    part = factor * lax.dot_general(
        tokens, back_pre, (((0,), (0,)), ((), ())), preferred_element_type=jnp.float32
    )

    @pl.when(step == 0)
    def _():
        g_ref[...] = part

    @pl.when(step > 0)
    def _():
        g_ref[...] += part


def local_gradient(which, current, tokens, targets, ids, frozen_out):
    pool, width = tokens.shape
    heads = current.shape[1]
    tile = tile_of(pool, 512)
    whole = lambda shape: pl.BlockSpec(shape, lambda i: (0, 0))
    return pl.pallas_call(
        functools.partial(gradient_body, which, tile, width ** (-0.5)),
        grid=(pool // tile,),
        in_specs=[
            whole(ids.shape),
            whole(current.shape),
            pl.BlockSpec((tile, width), lambda i: (i, 0)),
            pl.BlockSpec((tile, width), lambda i: (i, 0)),
            whole(frozen_out.shape),
        ],
        out_specs=whole((width, heads)),
        out_shape=jax.ShapeDtypeStruct((width, heads), jnp.float32),
        scratch_shapes=[pltpu.VMEM(current.shape, jnp.bfloat16)],
        compiler_params=pltpu.CompilerParams(
            dimension_semantics=("arbitrary",), vmem_limit_bytes=32 * 2**20
        ),
        cost_estimate=pl.CostEstimate(
            flops=8 * pool * width * heads, bytes_accessed=12 * 2**20, transcendentals=0
        ),
    )(ids, current, tokens, targets, frozen_out)


def add_body(weight_ref, rest_ref, piece_ref, out_ref):
    out_ref[...] = rest_ref[...] + weight_ref[0] * piece_ref[...]


def add_piece(weight, rest, piece, start):
    rows, heads = piece.shape
    tile = tile_of(rows, 128)
    first = start // tile
    return pl.pallas_call(
        add_body,
        grid=(rows // tile,),
        in_specs=[
            pl.BlockSpec(memory_space=pltpu.SMEM),
            pl.BlockSpec((tile, heads), lambda i: (i + first, 0)),
            pl.BlockSpec((tile, heads), lambda i: (i, 0)),
        ],
        out_specs=pl.BlockSpec((tile, heads), lambda i: (i + first, 0)),
        out_shape=jax.ShapeDtypeStruct(rest.shape, rest.dtype),
        input_output_aliases={1: 0},
        compiler_params=pltpu.CompilerParams(vmem_limit_bytes=4 * 2**20),
        cost_estimate=pl.CostEstimate(
            flops=2 * rows * heads, bytes_accessed=12 * rows * heads, transcendentals=0
        ),
        name="add_piece",
    )(weight, rest, piece)


def tail_body(start, weight_ref, filled_ref, rest_ref, piece_ref, out_ref, sum_ref, sem):
    sum_ref[...] = rest_ref[...] + weight_ref[0] * piece_ref[...]
    copy = pltpu.make_async_copy(sum_ref, out_ref.at[pl.ds(start, sum_ref.shape[0])], sem)
    copy.start()
    copy.wait()


def add_tail(weight, filled, rest, piece, start):
    rows, heads = piece.shape
    return pl.pallas_call(
        functools.partial(tail_body, start),
        in_specs=[
            pl.BlockSpec(memory_space=pltpu.SMEM),
            pl.BlockSpec(memory_space=pl.ANY),
            pl.BlockSpec(memory_space=pltpu.VMEM),
            pl.BlockSpec(memory_space=pltpu.VMEM),
        ],
        out_specs=pl.BlockSpec(memory_space=pl.ANY),
        out_shape=jax.ShapeDtypeStruct(filled.shape, filled.dtype),
        scratch_shapes=[pltpu.VMEM(piece.shape, piece.dtype), pltpu.SemaphoreType.DMA],
        input_output_aliases={1: 0},
        compiler_params=pltpu.CompilerParams(vmem_limit_bytes=4 * 2**20),
        cost_estimate=pl.CostEstimate(
            flops=2 * rows * heads, bytes_accessed=12 * rows * heads, transcendentals=0
        ),
        name="add_tail",
    )(weight, filled, rest, piece)


def track_body(spans, w_ref, own_ref, row_ref, col_ref, new_ref, old_ref, all_ref, *piece_refs):
    step = pl.program_id(0)
    mixed = w_ref[0] * own_ref[...] + w_ref[1] * row_ref[...] + w_ref[2] * col_ref[...]
    tracker = mixed + new_ref[...] - old_ref[...]
    all_ref[...] = tracker
    for (first, end), piece_ref in zip(spans, piece_refs):

        @pl.when((step >= first) & (step < end))
        def _():
            piece_ref[...] = tracker


def near_body(spans, w_ref, own_ref, row_ref, new_ref, old_ref, all_ref, *piece_refs):
    step = pl.program_id(0)
    near = w_ref[0] * own_ref[...] + w_ref[1] * row_ref[...] + (new_ref[...] - old_ref[...])
    all_ref[...] = near
    for (first, end), piece_ref in zip(spans, piece_refs):

        @pl.when((step >= first) & (step < end))
        def _():
            piece_ref[...] = near


def sweep(body, weights, arrays, cuts, tile):
    rows, heads = arrays[0].shape
    spans = [(a // tile, b // tile) for a, b in cuts]

    def piece_spec(first, end):
        return pl.BlockSpec((tile, heads), lambda i: (jnp.clip(i - first, 0, end - first - 1), 0))

    block = pl.BlockSpec((tile, heads), lambda i: (i, 0))
    return pl.pallas_call(
        functools.partial(body, spans),
        grid=(rows // tile,),
        in_specs=[pl.BlockSpec(memory_space=pltpu.SMEM)] + [block] * len(arrays),
        out_specs=[block] + [piece_spec(*span) for span in spans],
        out_shape=[jax.ShapeDtypeStruct((rows, heads), jnp.float32)]
        + [jax.ShapeDtypeStruct((b - a, heads), jnp.float32) for a, b in cuts],
        compiler_params=pltpu.CompilerParams(
            dimension_semantics=("arbitrary",), vmem_limit_bytes=8 * 2**20
        ),
        cost_estimate=pl.CostEstimate(
            flops=8 * rows * heads, bytes_accessed=28 * rows * heads, transcendentals=0
        ),
    )(weights, *arrays)


def combine(mix_weights, own, from_row, from_col):
    return mix_weights[0] * own + mix_weights[1] * from_row + mix_weights[2] * from_col


def on_device(value_proj, token_pool, target_pool, batch_ids, frozen_out, numerators):
    counts = numerators.astype(jnp.float32)
    mix_weights = counts / jnp.sum(counts)
    current = value_proj[0, 0]
    width = current.shape[0]
    tile = width // 8
    cuts = [(0, width // 2), (width // 2, width - tile), (width - tile, width)]

    def gradient_at(field, which):
        return local_gradient(
            which, field, token_pool[0, 0], target_pool[0, 0], batch_ids[0, 0], frozen_out
        )

    def neighbours(field):
        from_col = shifted(field, "col", 1)
        return shifted(field, "row", 1), from_col

    around_current = neighbours(current)
    grad_old = gradient_at(current, 0)
    tracker = grad_old
    for which in range(1, ITERS + 1):
        final = which == ITERS
        if which == 1:
            around_tracker = neighbours(tracker)
        current = combine(mix_weights, current, *around_current) - step_rate * tracker
        if not final:
            around_current = neighbours(current)
        grad_new = gradient_at(current, which)
        if not final:
            arrays = (tracker, *around_tracker, grad_new, grad_old)
            ends = cuts if which == ITERS - 1 else []
            tracker, *blocks = sweep(track_body, mix_weights, arrays, ends, tile)
            if which < ITERS - 1:
                around_tracker = neighbours(tracker)
            else:
                pieces = [shifted(b, "col", 1) for b in blocks]
                track_row = shifted(tracker, "row", 1)
            grad_old = grad_new

    arrays = (tracker, track_row, grad_new, grad_old)
    result, last = sweep(near_body, mix_weights, arrays, cuts[-1:], tile)
    for (start, _), piece in zip(cuts[:-1], pieces):
        result = add_piece(mix_weights[2:], result, piece, start)
    result = add_tail(mix_weights[2:], result, last, pieces[-1], cuts[-1][0])
    return (current[None, None], result[None, None])


def solution(mesh):
    whole = P("row", "col", None, None)
    return jax.shard_map(
        on_device,
        mesh=mesh,
        in_specs=(whole, whole, whole, whole, P(), P()),
        out_specs=(whole, whole),
        check_vma=False,
    )
```

```python
import functools

import jax
import jax.numpy as jnp
from jax import lax
from jax.experimental import pallas as pl
from jax.experimental.pallas import tpu as pltpu
from jax.sharding import PartitionSpec as P


ITERS = 2

step_rate = 0.2


def shifted(block, axis, distance):
    devices = range(lax.axis_size(axis))
    route = [((i - distance) % len(devices), i) for i in devices]
    return lax.ppermute(block, axis, route)


def tile_of(rows, most):
    tile = min(rows, most)
    while rows % tile:
        tile -= 8
    return tile


def gradient_body(which, tile, factor, ids_ref, x_ref, tok_ref, tgt_ref, out_ref, g_ref, xb_ref):
    step = pl.program_id(0)

    @pl.when(step == 0)
    def _():
        xb_ref[...] = x_ref[...].astype(jnp.bfloat16)

    tokens = tok_ref[...]
    frozen = out_ref[...]
    preact = jnp.dot(tokens, xb_ref[...], preferred_element_type=jnp.float32) * factor
    sigmoid_pre = jax.nn.sigmoid(preact)
    hidden = (preact * sigmoid_pre).astype(jnp.bfloat16)
    output = jnp.dot(hidden, frozen, preferred_element_type=jnp.float32)
    error_term = (output - tgt_ref[...].astype(jnp.float32)).astype(jnp.bfloat16)
    back_hidden = lax.dot_general(
        error_term, frozen, (((1,), (1,)), ((), ())), preferred_element_type=jnp.float32
    )
    slope = sigmoid_pre * (1.0 + preact * (1.0 - sigmoid_pre))
    rows = lax.broadcasted_iota(jnp.int32, (tile, ids_ref.shape[1]), 0) + step * tile
    named = jnp.where(rows == ids_ref[which : which + 1, :], 1.0, 0.0)
    times = jnp.sum(named, axis=1, keepdims=True)
    back_pre = (back_hidden * slope * times).astype(jnp.bfloat16)
    part = factor * lax.dot_general(
        tokens, back_pre, (((0,), (0,)), ((), ())), preferred_element_type=jnp.float32
    )

    @pl.when(step == 0)
    def _():
        g_ref[...] = part

    @pl.when(step > 0)
    def _():
        g_ref[...] += part


def local_gradient(which, current, tokens, targets, ids, frozen_out):
    pool, width = tokens.shape
    heads = current.shape[1]
    tile = tile_of(pool, 512)
    whole = lambda shape: pl.BlockSpec(shape, lambda i: (0, 0))
    return pl.pallas_call(
        functools.partial(gradient_body, which, tile, width ** (-0.5)),
        grid=(pool // tile,),
        in_specs=[
            whole(ids.shape),
            whole(current.shape),
            pl.BlockSpec((tile, width), lambda i: (i, 0)),
            pl.BlockSpec((tile, width), lambda i: (i, 0)),
            whole(frozen_out.shape),
        ],
        out_specs=whole((width, heads)),
        out_shape=jax.ShapeDtypeStruct((width, heads), jnp.float32),
        scratch_shapes=[pltpu.VMEM(current.shape, jnp.bfloat16)],
        compiler_params=pltpu.CompilerParams(
            dimension_semantics=("arbitrary",), vmem_limit_bytes=32 * 2**20
        ),
        cost_estimate=pl.CostEstimate(
            flops=8 * pool * width * heads, bytes_accessed=12 * 2**20, transcendentals=0
        ),
    )(ids, current, tokens, targets, frozen_out)


def add_body(rest_ref, piece_ref, out_ref):
    out_ref[...] = rest_ref[...] + piece_ref[...]


def add_piece(rest, piece, start):
    rows, heads = piece.shape
    tile = tile_of(rows, 128)
    first = start // tile
    return pl.pallas_call(
        add_body,
        grid=(rows // tile,),
        in_specs=[
            pl.BlockSpec((tile, heads), lambda i: (i + first, 0)),
            pl.BlockSpec((tile, heads), lambda i: (i, 0)),
        ],
        out_specs=pl.BlockSpec((tile, heads), lambda i: (i + first, 0)),
        out_shape=jax.ShapeDtypeStruct(rest.shape, rest.dtype),
        input_output_aliases={0: 0},
        compiler_params=pltpu.CompilerParams(vmem_limit_bytes=4 * 2**20),
        cost_estimate=pl.CostEstimate(
            flops=2 * rows * heads, bytes_accessed=12 * rows * heads, transcendentals=0
        ),
        name="add_piece",
    )(rest, piece)


def tail_body(start, filled_ref, rest_ref, piece_ref, out_ref, sum_ref, sem):
    sum_ref[...] = rest_ref[...] + piece_ref[...]
    copy = pltpu.make_async_copy(sum_ref, out_ref.at[pl.ds(start, sum_ref.shape[0])], sem)
    copy.start()
    copy.wait()


def add_tail(filled, rest, piece, start):
    rows, heads = piece.shape
    return pl.pallas_call(
        functools.partial(tail_body, start),
        in_specs=[
            pl.BlockSpec(memory_space=pl.ANY),
            pl.BlockSpec(memory_space=pltpu.VMEM),
            pl.BlockSpec(memory_space=pltpu.VMEM),
        ],
        out_specs=pl.BlockSpec(memory_space=pl.ANY),
        out_shape=jax.ShapeDtypeStruct(filled.shape, filled.dtype),
        scratch_shapes=[pltpu.VMEM(piece.shape, piece.dtype), pltpu.SemaphoreType.DMA],
        input_output_aliases={0: 0},
        compiler_params=pltpu.CompilerParams(vmem_limit_bytes=4 * 2**20),
        cost_estimate=pl.CostEstimate(
            flops=2 * rows * heads, bytes_accessed=12 * rows * heads, transcendentals=0
        ),
        name="add_tail",
    )(filled, rest, piece)


def track_body(spans, w_ref, own_ref, row_ref, col_ref, new_ref, old_ref, all_ref, *piece_refs):
    step = pl.program_id(0)
    mixed = w_ref[0] * own_ref[...] + w_ref[1] * row_ref[...] + w_ref[2] * col_ref[...]
    tracker = mixed + new_ref[...] - old_ref[...]
    all_ref[...] = tracker
    for (first, end), piece_ref in zip(spans, piece_refs):

        @pl.when((step >= first) & (step < end))
        def _():
            piece_ref[...] = w_ref[2] * tracker


def near_body(spans, w_ref, own_ref, row_ref, new_ref, old_ref, all_ref, *piece_refs):
    step = pl.program_id(0)
    near = w_ref[0] * own_ref[...] + w_ref[1] * row_ref[...] + (new_ref[...] - old_ref[...])
    all_ref[...] = near
    for (first, end), piece_ref in zip(spans, piece_refs):

        @pl.when((step >= first) & (step < end))
        def _():
            piece_ref[...] = near


def sweep(body, weights, arrays, cuts, tile):
    rows, heads = arrays[0].shape
    spans = [(a // tile, b // tile) for a, b in cuts]

    def piece_spec(first, end):
        return pl.BlockSpec((tile, heads), lambda i: (jnp.clip(i - first, 0, end - first - 1), 0))

    block = pl.BlockSpec((tile, heads), lambda i: (i, 0))
    return pl.pallas_call(
        functools.partial(body, spans),
        grid=(rows // tile,),
        in_specs=[pl.BlockSpec(memory_space=pltpu.SMEM)] + [block] * len(arrays),
        out_specs=[block] + [piece_spec(*span) for span in spans],
        out_shape=[jax.ShapeDtypeStruct((rows, heads), jnp.float32)]
        + [jax.ShapeDtypeStruct((b - a, heads), jnp.float32) for a, b in cuts],
        compiler_params=pltpu.CompilerParams(
            dimension_semantics=("arbitrary",), vmem_limit_bytes=8 * 2**20
        ),
        cost_estimate=pl.CostEstimate(
            flops=8 * rows * heads, bytes_accessed=28 * rows * heads, transcendentals=0
        ),
    )(weights, *arrays)


def combine(mix_weights, own, from_row, from_col):
    return mix_weights[0] * own + mix_weights[1] * from_row + mix_weights[2] * from_col


def on_device(value_proj, token_pool, target_pool, batch_ids, frozen_out, numerators):
    counts = numerators.astype(jnp.float32)
    mix_weights = counts / jnp.sum(counts)
    current = value_proj[0, 0]
    width = current.shape[0]
    tile = width // 8
    cuts = [(0, width // 2), (width // 2, width - tile), (width - tile, width)]

    def gradient_at(field, which):
        return local_gradient(
            which, field, token_pool[0, 0], target_pool[0, 0], batch_ids[0, 0], frozen_out
        )

    def neighbours(field):
        from_col = shifted(field, "col", 1)
        return shifted(field, "row", 1), from_col

    around_current = neighbours(current)
    grad_old = gradient_at(current, 0)
    tracker = grad_old
    for which in range(1, ITERS + 1):
        final = which == ITERS
        if which == 1:
            around_tracker = neighbours(tracker)
        current = combine(mix_weights, current, *around_current) - step_rate * tracker
        if not final:
            around_current = neighbours(current)
        grad_new = gradient_at(current, which)
        if not final:
            arrays = (tracker, *around_tracker, grad_new, grad_old)
            ends = cuts if which == ITERS - 1 else []
            tracker, *blocks = sweep(track_body, mix_weights, arrays, ends, tile)
            if which < ITERS - 1:
                around_tracker = neighbours(tracker)
            else:
                pieces = [shifted(b, "col", 1) for b in blocks]
                track_row = shifted(tracker, "row", 1)
            grad_old = grad_new

    arrays = (tracker, track_row, grad_new, grad_old)
    result, last = sweep(near_body, mix_weights, arrays, cuts[-1:], tile)
    for (start, _), piece in zip(cuts[:-1], pieces):
        result = add_piece(result, piece, start)
    result = add_tail(result, last, pieces[-1], cuts[-1][0])
    return (current[None, None], result[None, None])


def solution(mesh):
    whole = P("row", "col", None, None)
    return jax.shard_map(
        on_device,
        mesh=mesh,
        in_specs=(whole, whole, whole, whole, P(), P()),
        out_specs=(whole, whole),
        check_vma=False,
    )
```

```python
import functools

import jax
import jax.numpy as jnp
from jax import lax
from jax.experimental import pallas as pl
from jax.experimental.pallas import tpu as pltpu
from jax.sharding import PartitionSpec as P


step_rate = 0.2


def shifted(block, axis, distance, wraps=True):
    devices = range(lax.axis_size(axis))
    route = [((i - distance) % len(devices), i) for i in devices if wraps or i >= distance]
    return lax.ppermute(block, axis, route)


def last_to_second(block, axis):
    size = lax.axis_size(axis)
    return lax.ppermute(block, axis, [(size - 1, 1 % size)])


def tile_of(rows, most):
    tile = min(rows, most)
    while rows % tile:
        tile -= 8
    return tile


def gradient_body(which, tile, factor, ids_ref, x_ref, tok_ref, tgt_ref, out_ref, g_ref, xb_ref):
    step = pl.program_id(0)

    @pl.when(step == 0)
    def _():
        xb_ref[...] = x_ref[...].astype(jnp.bfloat16)

    tokens = tok_ref[...]
    frozen = out_ref[...]
    preact = jnp.dot(tokens, xb_ref[...], preferred_element_type=jnp.float32) * factor
    sigmoid_pre = jax.nn.sigmoid(preact)
    hidden = (preact * sigmoid_pre).astype(jnp.bfloat16)
    output = jnp.dot(hidden, frozen, preferred_element_type=jnp.float32)
    error_term = (output - tgt_ref[...].astype(jnp.float32)).astype(jnp.bfloat16)
    back_hidden = lax.dot_general(
        error_term, frozen, (((1,), (1,)), ((), ())), preferred_element_type=jnp.float32
    )
    slope = sigmoid_pre * (1.0 + preact * (1.0 - sigmoid_pre))
    rows = lax.broadcasted_iota(jnp.int32, (tile, ids_ref.shape[1]), 0) + step * tile
    named = jnp.where(rows == ids_ref[which : which + 1, :], 1.0, 0.0)
    times = jnp.sum(named, axis=1, keepdims=True)
    back_pre = (back_hidden * slope * times).astype(jnp.bfloat16)
    part = factor * lax.dot_general(
        tokens, back_pre, (((0,), (0,)), ((), ())), preferred_element_type=jnp.float32
    )

    @pl.when(step == 0)
    def _():
        g_ref[...] = part

    @pl.when(step > 0)
    def _():
        g_ref[...] += part


def local_gradient(which, current, tokens, targets, ids, frozen_out):
    pool, width = tokens.shape
    heads = current.shape[1]
    tile = tile_of(pool, 512)
    whole = lambda shape: pl.BlockSpec(shape, lambda i: (0, 0))
    return pl.pallas_call(
        functools.partial(gradient_body, which, tile, width ** (-0.5)),
        grid=(pool // tile,),
        in_specs=[
            whole(ids.shape),
            whole(current.shape),
            pl.BlockSpec((tile, width), lambda i: (i, 0)),
            pl.BlockSpec((tile, width), lambda i: (i, 0)),
            whole(frozen_out.shape),
        ],
        out_specs=whole((width, heads)),
        out_shape=jax.ShapeDtypeStruct((width, heads), jnp.float32),
        scratch_shapes=[pltpu.VMEM(current.shape, jnp.bfloat16)],
        compiler_params=pltpu.CompilerParams(
            dimension_semantics=("arbitrary",), vmem_limit_bytes=32 * 2**20
        ),
        cost_estimate=pl.CostEstimate(
            flops=8 * pool * width * heads, bytes_accessed=12 * 2**20, transcendentals=0
        ),
    )(ids, current, tokens, targets, frozen_out)


def add_body(rest_ref, piece_ref, out_ref):
    out_ref[...] = rest_ref[...] + piece_ref[...]


def add_piece(rest, piece, start):
    rows, heads = piece.shape
    tile = tile_of(rows, 128)
    first = start // tile
    return pl.pallas_call(
        add_body,
        grid=(rows // tile,),
        in_specs=[
            pl.BlockSpec((tile, heads), lambda i: (i + first, 0)),
            pl.BlockSpec((tile, heads), lambda i: (i, 0)),
        ],
        out_specs=pl.BlockSpec((tile, heads), lambda i: (i + first, 0)),
        out_shape=jax.ShapeDtypeStruct(rest.shape, rest.dtype),
        input_output_aliases={0: 0},
        compiler_params=pltpu.CompilerParams(vmem_limit_bytes=4 * 2**20),
        cost_estimate=pl.CostEstimate(
            flops=2 * rows * heads, bytes_accessed=12 * rows * heads, transcendentals=0
        ),
        name="add_piece",
    )(rest, piece)


def tail_body(start, filled_ref, rest_ref, piece_ref, far_ref, out_ref, sum_ref, sem):
    sum_ref[...] = rest_ref[...] + piece_ref[...] + far_ref[...]
    copy = pltpu.make_async_copy(sum_ref, out_ref.at[pl.ds(start, sum_ref.shape[0])], sem)
    copy.start()
    copy.wait()


def add_tail(filled, rest, piece, far, start):
    rows, heads = piece.shape
    return pl.pallas_call(
        functools.partial(tail_body, start),
        in_specs=[
            pl.BlockSpec(memory_space=pl.ANY),
            pl.BlockSpec(memory_space=pltpu.VMEM),
            pl.BlockSpec(memory_space=pltpu.VMEM),
            pl.BlockSpec(memory_space=pltpu.VMEM),
        ],
        out_specs=pl.BlockSpec(memory_space=pl.ANY),
        out_shape=jax.ShapeDtypeStruct(filled.shape, filled.dtype),
        scratch_shapes=[pltpu.VMEM(piece.shape, piece.dtype), pltpu.SemaphoreType.DMA],
        input_output_aliases={0: 0},
        compiler_params=pltpu.CompilerParams(vmem_limit_bytes=4 * 2**20),
        cost_estimate=pl.CostEstimate(
            flops=2 * rows * heads, bytes_accessed=12 * rows * heads, transcendentals=0
        ),
        name="add_tail",
    )(filled, rest, piece, far)


def step_sum(w, lead, own, from_row, from_col, tracker):
    moved = w[0] * own + w[1] * from_row + w[2] * from_col - step_rate * tracker
    return moved, moved - jnp.where(lead, step_rate * w[3], 0.0) * tracker


def track_sum(w, lead, own, from_row, from_col, new, old):
    tracker = w[0] * own + w[1] * from_row + w[2] * from_col + new - old
    extra = jnp.where(lead, w[3], 0.0) * (w[0] * own + w[1] * from_row)
    return tracker, w[2] * (tracker + extra)


def near_sum(w, lead, own, from_row, new, old):
    near = w[0] * own + w[1] * from_row + (new - old)
    return near, near


def sweep_body(formula, split, spans, w_ref, *refs):
    step = pl.program_id(0)
    values, at = [], 0
    for parts in split:
        value = refs[at][...]
        if parts == 2:
            value = jnp.where(step == 0, value, refs[at + 1][...])
        values.append(value)
        at += parts
    result, other = formula([w_ref[i] for i in range(4)], step == 0, *values)
    refs[at][...] = result
    for (first, end), piece_ref in zip(spans, refs[at + 1 :]):

        @pl.when((step >= first) & (step < end))
        def _():
            piece_ref[...] = other


def sweep(formula, weights, arrays, cuts, tile):
    rows, heads = arrays[0].shape
    spans = [(a // tile, b // tile) for a, b in cuts]

    def part(first, end):
        return pl.BlockSpec((tile, heads), lambda i: (jnp.clip(i - first, 0, end - first - 1), 0))

    steps = rows // tile
    specs, flat, split = [], [], []
    for array in arrays:
        if isinstance(array, tuple):
            specs += [part(0, 1), part(1, steps)]
            flat += array
            split.append(2)
        else:
            specs.append(part(0, steps))
            flat.append(array)
            split.append(1)
    return pl.pallas_call(
        functools.partial(sweep_body, formula, split, spans),
        grid=(steps,),
        in_specs=[pl.BlockSpec(memory_space=pltpu.SMEM)] + specs,
        out_specs=[part(0, steps)] + [part(*span) for span in spans],
        out_shape=[jax.ShapeDtypeStruct((rows, heads), jnp.float32)]
        + [jax.ShapeDtypeStruct((b - a, heads), jnp.float32) for a, b in cuts],
        compiler_params=pltpu.CompilerParams(
            dimension_semantics=("arbitrary",), vmem_limit_bytes=8 * 2**20
        ),
        cost_estimate=pl.CostEstimate(
            flops=8 * rows * heads, bytes_accessed=28 * rows * heads, transcendentals=0
        ),
    )(weights, *flat)


def on_device(value_proj, token_pool, target_pool, batch_ids, frozen_out, numerators):
    counts = numerators.astype(jnp.float32)
    is_last = lax.axis_index("col") == lax.axis_size("col") - 1
    mix_weights = counts / jnp.sum(counts)
    weights = jnp.concatenate([mix_weights, is_last.astype(jnp.float32)[None]])
    x0 = value_proj[0, 0]
    width = x0.shape[0]
    lead = width // 8
    middle = width * 5 // 8
    cuts = [(lead, middle), (middle, width), (0, lead)]

    def gradient_at(field, which):
        return local_gradient(
            which, field, token_pool[0, 0], target_pool[0, 0], batch_ids[0, 0], frozen_out
        )

    x0_col = shifted(x0, "col", 1)
    x0_row = shifted(x0, "row", 1)
    g0 = gradient_at(x0, 0)
    g0_rest, g0_lead = lax.optimization_barrier((g0[lead:], g0[:lead]))
    g0_col = (shifted(g0_lead, "col", 1, wraps=False), shifted(g0_rest, "col", 1))
    g0_row = shifted(g0, "row", 1)

    x1, x1_send = sweep(step_sum, weights, (x0, x0_row, x0_col, g0), [(0, width)], lead)
    x1_col = shifted(x1_send, "col", 1)
    x1_row = shifted(x1, "row", 1)
    g1 = gradient_at(x1, 1)

    arrays = (g0, g0_row, g0_col, g1, g0)
    t1, *blocks = sweep(track_sum, weights, arrays, cuts, lead)
    pieces = [shifted(block, "col", 1) for block in blocks]
    far = last_to_second(mix_weights[2] * mix_weights[2] * g0_lead, "col")
    t1_row = shifted(t1, "row", 1)

    (x2,) = sweep(step_sum, weights, (x1, x1_row, x1_col, t1), [], lead)
    g2 = gradient_at(x2, 2)

    t2, last = sweep(near_sum, weights, (t1, t1_row, g2, g1), cuts[-1:], lead)
    for (start, _), piece in zip(cuts[:-1], pieces):
        t2 = add_piece(t2, piece, start)
    t2 = add_tail(t2, last, pieces[-1], far, cuts[-1][0])
    return (x2[None, None], t2[None, None])


def solution(mesh):
    whole = P("row", "col", None, None)
    return jax.shard_map(
        on_device,
        mesh=mesh,
        in_specs=(whole, whole, whole, whole, P(), P()),
        out_specs=(whole, whole),
        check_vma=False,
    )
```

```python
import functools

import jax
import jax.numpy as jnp
from jax import lax
from jax.experimental import pallas as pl
from jax.experimental.pallas import tpu as pltpu
from jax.sharding import PartitionSpec as P


step_rate = 0.2

SUMS_VMEM = 24 * 2**20


def shifted(block, axis, distance, wraps=True):
    devices = range(lax.axis_size(axis))
    route = [((i - distance) % len(devices), i) for i in devices if wraps or i >= distance]
    return lax.ppermute(block, axis, route)


def last_to_second(block, axis):
    size = lax.axis_size(axis)
    return lax.ppermute(block, axis, [(size - 1, 1 % size)])


def tile_of(rows, most):
    tile = min(rows, most)
    while rows % tile:
        tile -= 8
    return tile


def gradient_body(which, tile, factor, ids_ref, x_ref, tok_ref, tgt_ref, out_ref, g_ref, xb_ref):
    step = pl.program_id(0)

    @pl.when(step == 0)
    def _():
        xb_ref[...] = x_ref[...].astype(jnp.bfloat16)

    tokens = tok_ref[...]
    frozen = out_ref[...]
    preact = jnp.dot(tokens, xb_ref[...], preferred_element_type=jnp.float32) * factor
    sigmoid_pre = jax.nn.sigmoid(preact)
    hidden = (preact * sigmoid_pre).astype(jnp.bfloat16)
    output = jnp.dot(hidden, frozen, preferred_element_type=jnp.float32)
    error_term = (output - tgt_ref[...].astype(jnp.float32)).astype(jnp.bfloat16)
    back_hidden = lax.dot_general(
        error_term, frozen, (((1,), (1,)), ((), ())), preferred_element_type=jnp.float32
    )
    slope = sigmoid_pre * (1.0 + preact * (1.0 - sigmoid_pre))
    rows = lax.broadcasted_iota(jnp.int32, (tile, ids_ref.shape[1]), 0) + step * tile
    named = jnp.where(rows == ids_ref[which : which + 1, :], 1.0, 0.0)
    times = jnp.sum(named, axis=1, keepdims=True)
    back_pre = (back_hidden * slope * times).astype(jnp.bfloat16)
    part = factor * lax.dot_general(
        tokens, back_pre, (((0,), (0,)), ((), ())), preferred_element_type=jnp.float32
    )

    @pl.when(step == 0)
    def _():
        g_ref[...] = part

    @pl.when(step > 0)
    def _():
        g_ref[...] += part


def local_gradient(which, current, tokens, targets, ids, frozen_out):
    pool, width = tokens.shape
    heads = current.shape[1]
    tile = tile_of(pool, 512)
    whole = lambda shape: pl.BlockSpec(shape, lambda i: (0, 0))
    return pl.pallas_call(
        functools.partial(gradient_body, which, tile, width ** (-0.5)),
        grid=(pool // tile,),
        in_specs=[
            whole(ids.shape),
            whole(current.shape),
            pl.BlockSpec((tile, width), lambda i: (i, 0)),
            pl.BlockSpec((tile, width), lambda i: (i, 0)),
            whole(frozen_out.shape),
        ],
        out_specs=whole((width, heads)),
        out_shape=jax.ShapeDtypeStruct((width, heads), jnp.float32),
        scratch_shapes=[pltpu.VMEM(current.shape, jnp.bfloat16)],
        compiler_params=pltpu.CompilerParams(
            dimension_semantics=("arbitrary",), vmem_limit_bytes=20 * 2**20
        ),
        cost_estimate=pl.CostEstimate(
            flops=8 * pool * width * heads, bytes_accessed=12 * 2**20, transcendentals=0
        ),
    )(ids, current, tokens, targets, frozen_out)


def add_body(rest_ref, piece_ref, out_ref):
    out_ref[...] = rest_ref[...] + piece_ref[...]


def add_piece(rest, piece, start):
    rows, heads = piece.shape
    tile = tile_of(rows, 128)
    first = start // tile
    return pl.pallas_call(
        add_body,
        grid=(rows // tile,),
        in_specs=[
            pl.BlockSpec((tile, heads), lambda i: (i + first, 0)),
            pl.BlockSpec((tile, heads), lambda i: (i, 0)),
        ],
        out_specs=pl.BlockSpec((tile, heads), lambda i: (i + first, 0)),
        out_shape=jax.ShapeDtypeStruct(rest.shape, rest.dtype),
        input_output_aliases={0: 0},
        compiler_params=pltpu.CompilerParams(vmem_limit_bytes=4 * 2**20),
        cost_estimate=pl.CostEstimate(
            flops=2 * rows * heads, bytes_accessed=12 * rows * heads, transcendentals=0
        ),
        name="add_piece",
    )(rest, piece)


def tail_body(start, filled_ref, rest_ref, piece_ref, far_ref, out_ref, sum_ref, sem):
    sum_ref[...] = rest_ref[...] + piece_ref[...] + far_ref[...]
    copy = pltpu.make_async_copy(sum_ref, out_ref.at[pl.ds(start, sum_ref.shape[0])], sem)
    copy.start()
    copy.wait()


def add_tail(filled, rest, piece, far, start):
    rows, heads = piece.shape
    return pl.pallas_call(
        functools.partial(tail_body, start),
        in_specs=[
            pl.BlockSpec(memory_space=pl.ANY),
            pl.BlockSpec(memory_space=pltpu.VMEM),
            pl.BlockSpec(memory_space=pltpu.VMEM),
            pl.BlockSpec(memory_space=pltpu.VMEM),
        ],
        out_specs=pl.BlockSpec(memory_space=pl.ANY),
        out_shape=jax.ShapeDtypeStruct(filled.shape, filled.dtype),
        scratch_shapes=[pltpu.VMEM(piece.shape, piece.dtype), pltpu.SemaphoreType.DMA],
        input_output_aliases={0: 0},
        compiler_params=pltpu.CompilerParams(vmem_limit_bytes=4 * 2**20),
        cost_estimate=pl.CostEstimate(
            flops=2 * rows * heads, bytes_accessed=12 * rows * heads, transcendentals=0
        ),
        name="add_tail",
    )(filled, rest, piece, far)


def step_sum(w, lead, own, from_row, from_col, tracker):
    moved = w[0] * own + w[1] * from_row + w[2] * from_col - step_rate * tracker
    return moved, moved - step_rate * w[3] * tracker if lead else moved


def plain_step(w, lead, own, from_row, from_col, tracker):
    return (step_sum(w, False, own, from_row, from_col, tracker)[0],) * 2


def track_sum(w, lead, own, from_row, from_col, new, old):
    tracker = w[0] * own + w[1] * from_row + w[2] * from_col + new - old
    extra = w[3] * (w[0] * own + w[1] * from_row) if lead else 0.0
    return tracker, w[2] * (tracker + extra)


def sums_body(formula, split, cuts, tile, w_ref, *refs):
    w = [w_ref[i] for i in range(4)]
    first_out = sum(split)
    for start in range(0, refs[first_out].shape[0], tile):
        values, at = [], 0
        for parts in split:
            if parts == 1:
                values.append(refs[at][pl.ds(start, tile)])
            elif start == 0:
                values.append(refs[at][...])
            else:
                values.append(refs[at + 1][pl.ds(start - tile, tile)])
            at += parts
        result, other = formula(w, start == 0, *values)
        refs[at][pl.ds(start, tile)] = result
        for (a, b), piece_ref in zip(cuts, refs[at + 1 :]):
            if a <= start < b:
                piece_ref[pl.ds(start - a, tile)] = other


def sums(formula, weights, arrays, cuts, tile):
    rows, heads = arrays[0].shape
    split = [len(array) if isinstance(array, tuple) else 1 for array in arrays]
    flat = jax.tree.leaves(list(arrays))
    held = pl.BlockSpec(memory_space=pltpu.VMEM)
    return pl.pallas_call(
        functools.partial(sums_body, formula, split, cuts, tile),
        in_specs=[pl.BlockSpec(memory_space=pltpu.SMEM)] + [held] * len(flat),
        out_specs=[held] * (1 + len(cuts)),
        out_shape=[jax.ShapeDtypeStruct((rows, heads), jnp.float32)]
        + [jax.ShapeDtypeStruct((b - a, heads), jnp.float32) for a, b in cuts],
        compiler_params=pltpu.CompilerParams(vmem_limit_bytes=SUMS_VMEM),
        cost_estimate=pl.CostEstimate(
            flops=8 * rows * heads, bytes_accessed=28 * rows * heads, transcendentals=0
        ),
    )(weights, *flat)


def near_body(w_ref, own_ref, row_ref, new_ref, old_ref, near_ref, lead_ref):
    near = w_ref[0] * own_ref[...] + w_ref[1] * row_ref[...] + (new_ref[...] - old_ref[...])
    near_ref[...] = near

    @pl.when(pl.program_id(0) == 0)
    def _():
        lead_ref[...] = near


def near_sums(weights, arrays, tile):
    rows, heads = arrays[0].shape
    block = pl.BlockSpec((tile, heads), lambda i: (i, 0))
    return pl.pallas_call(
        near_body,
        grid=(rows // tile,),
        in_specs=[pl.BlockSpec(memory_space=pltpu.SMEM)] + [block] * len(arrays),
        out_specs=[block, pl.BlockSpec((tile, heads), lambda i: (0, 0))],
        out_shape=[
            jax.ShapeDtypeStruct((rows, heads), jnp.float32),
            jax.ShapeDtypeStruct((tile, heads), jnp.float32),
        ],
        compiler_params=pltpu.CompilerParams(
            dimension_semantics=("arbitrary",), vmem_limit_bytes=8 * 2**20
        ),
        cost_estimate=pl.CostEstimate(
            flops=8 * rows * heads, bytes_accessed=24 * rows * heads, transcendentals=0
        ),
        name="near",
    )(weights, *arrays)


def on_device(value_proj, token_pool, target_pool, batch_ids, frozen_out, numerators):
    counts = numerators.astype(jnp.float32)
    is_last = lax.axis_index("col") == lax.axis_size("col") - 1
    mix_weights = counts / jnp.sum(counts)
    weights = jnp.concatenate([mix_weights, is_last.astype(jnp.float32)[None]])
    x0 = value_proj[0, 0]
    width = x0.shape[0]
    lead = width // 8
    middle = width * 5 // 8
    cuts = [(lead, middle), (middle, width), (0, lead)]

    def gradient_at(field, which):
        return local_gradient(
            which, field, token_pool[0, 0], target_pool[0, 0], batch_ids[0, 0], frozen_out
        )

    x0_col = shifted(x0, "col", 1)
    x0_row = shifted(x0, "row", 1)
    g0 = gradient_at(x0, 0)
    g0_rest, g0_lead = lax.optimization_barrier((g0[lead:], g0[:lead]))
    g0_col = (shifted(g0_lead, "col", 1, wraps=False), shifted(g0_rest, "col", 1))
    g0_row = shifted(g0, "row", 1)

    x1, x1_send = sums(step_sum, weights, (x0, x0_row, x0_col, g0), [(0, width)], lead)
    x1_col = shifted(x1_send, "col", 1)
    x1_row = shifted(x1, "row", 1)
    g1 = gradient_at(x1, 1)

    arrays = (g0, g0_row, g0_col, g1, g0)
    t1, *blocks = sums(track_sum, weights, arrays, cuts, lead)
    pieces = [shifted(block, "col", 1) for block in blocks]
    far = last_to_second(mix_weights[2] * mix_weights[2] * g0_lead, "col")
    t1_row = shifted(t1, "row", 1)

    x2, x2_out = sums(plain_step, weights, (x1, x1_row, x1_col, t1), [(0, width)], lead)
    g2 = gradient_at(x2, 2)

    t2, last = near_sums(weights, (t1, t1_row, g2, g1), lead)
    for (start, _), piece in zip(cuts[:-1], pieces):
        t2 = add_piece(t2, piece, start)
    t2 = add_tail(t2, last, pieces[-1], far, cuts[-1][0])
    return (x2_out[None, None], t2[None, None])


def solution(mesh):
    whole = P("row", "col", None, None)
    return jax.shard_map(
        on_device,
        mesh=mesh,
        in_specs=(whole, whole, whole, whole, P(), P()),
        out_specs=(whole, whole),
        check_vma=False,
    )
```

```python
import functools
import math

import jax
import jax.numpy as jnp
from jax import lax
from jax.experimental import pallas as pl
from jax.experimental.pallas import tpu as pltpu
from jax.sharding import PartitionSpec as P


step_rate = 0.2

SUMS_VMEM = 24 * 2**20


def shifted(block, axis, distance, wraps=True):
    devices = range(lax.axis_size(axis))
    route = [((i - distance) % len(devices), i) for i in devices if wraps or i >= distance]
    return lax.ppermute(block, axis, route)


def last_to_second(block, axis):
    size = lax.axis_size(axis)
    return lax.ppermute(block, axis, [(size - 1, 1 % size)])


def tile_of(rows, most):
    tile = min(rows, most)
    while rows % tile:
        tile -= 8
    return tile


def gradient_body(which, tile, factor, ids_ref, x_ref, tok_ref, tgt_ref, out_ref, g_ref, xb_ref):
    step = pl.program_id(0)

    @pl.when(step == 0)
    def _():
        xb_ref[...] = x_ref[...].astype(jnp.bfloat16)

    tokens = tok_ref[...]
    frozen = out_ref[...]
    preact = jnp.dot(tokens, xb_ref[...], preferred_element_type=jnp.float32) * factor
    sigmoid_pre = jax.nn.sigmoid(preact)
    hidden = (preact * sigmoid_pre).astype(jnp.bfloat16)
    output = jnp.dot(hidden, frozen, preferred_element_type=jnp.float32)
    error_term = (output - tgt_ref[...].astype(jnp.float32)).astype(jnp.bfloat16)
    back_hidden = lax.dot_general(
        error_term, frozen, (((1,), (1,)), ((), ())), preferred_element_type=jnp.float32
    )
    slope = sigmoid_pre * (1.0 + preact * (1.0 - sigmoid_pre))
    rows = lax.broadcasted_iota(jnp.int32, (tile, ids_ref.shape[1]), 0) + step * tile
    named = jnp.where(rows == ids_ref[which : which + 1, :], 1.0, 0.0)
    times = jnp.sum(named, axis=1, keepdims=True)
    back_pre = (back_hidden * slope * times).astype(jnp.bfloat16)
    part = factor * lax.dot_general(
        tokens, back_pre, (((0,), (0,)), ((), ())), preferred_element_type=jnp.float32
    )

    @pl.when(step == 0)
    def _():
        g_ref[...] = part

    @pl.when(step > 0)
    def _():
        g_ref[...] += part


def local_gradient(which, current, tokens, targets, ids, frozen_out):
    pool, width = tokens.shape
    heads = current.shape[1]
    tile = tile_of(pool, 512)
    whole = lambda shape: pl.BlockSpec(shape, lambda i: (0, 0))
    return pl.pallas_call(
        functools.partial(gradient_body, which, tile, width ** (-0.5)),
        grid=(pool // tile,),
        in_specs=[
            whole(ids.shape),
            whole(current.shape),
            pl.BlockSpec((tile, width), lambda i: (i, 0)),
            pl.BlockSpec((tile, width), lambda i: (i, 0)),
            whole(frozen_out.shape),
        ],
        out_specs=whole((width, heads)),
        out_shape=jax.ShapeDtypeStruct((width, heads), jnp.float32),
        scratch_shapes=[pltpu.VMEM(current.shape, jnp.bfloat16)],
        compiler_params=pltpu.CompilerParams(
            dimension_semantics=("arbitrary",), vmem_limit_bytes=(20 if which else 60) * 2**20
        ),
        cost_estimate=pl.CostEstimate(
            flops=8 * pool * width * heads, bytes_accessed=12 * 2**20, transcendentals=0
        ),
    )(ids, current, tokens, targets, frozen_out)


def add_body(rest_ref, piece_ref, out_ref):
    out_ref[...] = rest_ref[...] + piece_ref[...]


def add_piece(rest, piece, start):
    rows, heads = piece.shape
    tile = tile_of(math.gcd(rows, start), 128)
    first = start // tile
    return pl.pallas_call(
        add_body,
        grid=(rows // tile,),
        in_specs=[
            pl.BlockSpec((tile, heads), lambda i: (i + first, 0)),
            pl.BlockSpec((tile, heads), lambda i: (i, 0)),
        ],
        out_specs=pl.BlockSpec((tile, heads), lambda i: (i + first, 0)),
        out_shape=jax.ShapeDtypeStruct(rest.shape, rest.dtype),
        input_output_aliases={0: 0},
        compiler_params=pltpu.CompilerParams(vmem_limit_bytes=4 * 2**20),
        cost_estimate=pl.CostEstimate(
            flops=2 * rows * heads, bytes_accessed=12 * rows * heads, transcendentals=0
        ),
        name="add_piece",
    )(rest, piece)


def tail_body(start, filled_ref, rest_ref, piece_ref, far_ref, out_ref, sum_ref, sem):
    sum_ref[...] = rest_ref[...] + piece_ref[...] + far_ref[...]
    copy = pltpu.make_async_copy(sum_ref, out_ref.at[pl.ds(start, sum_ref.shape[0])], sem)
    copy.start()
    copy.wait()


def add_tail(filled, rest, piece, far, start):
    rows, heads = piece.shape
    return pl.pallas_call(
        functools.partial(tail_body, start),
        in_specs=[
            pl.BlockSpec(memory_space=pl.ANY),
            pl.BlockSpec(memory_space=pltpu.VMEM),
            pl.BlockSpec(memory_space=pltpu.VMEM),
            pl.BlockSpec(memory_space=pltpu.VMEM),
        ],
        out_specs=pl.BlockSpec(memory_space=pl.ANY),
        out_shape=jax.ShapeDtypeStruct(filled.shape, filled.dtype),
        scratch_shapes=[pltpu.VMEM(piece.shape, piece.dtype), pltpu.SemaphoreType.DMA],
        input_output_aliases={0: 0},
        compiler_params=pltpu.CompilerParams(vmem_limit_bytes=4 * 2**20),
        cost_estimate=pl.CostEstimate(
            flops=2 * rows * heads, bytes_accessed=12 * rows * heads, transcendentals=0
        ),
        name="add_tail",
    )(filled, rest, piece, far)


def step_sum(w, lead, own, from_row, from_col, tracker):
    moved = w[0] * own + w[1] * from_row + w[2] * from_col - step_rate * tracker
    return moved, moved - step_rate * w[3] * tracker if lead else moved


def plain_step(w, lead, own, from_row, from_col, tracker):
    return (step_sum(w, False, own, from_row, from_col, tracker)[0],) * 2


def track_sum(w, lead, own, from_row, from_col, new, old):
    tracker = w[0] * own + w[1] * from_row + w[2] * from_col + new - old
    extra = w[3] * (w[0] * own + w[1] * from_row) if lead else 0.0
    return tracker, w[2] * (tracker + extra)


def sums_body(formula, split, cuts, tile, w_ref, *refs):
    w = [w_ref[i] for i in range(4)]
    first_out = sum(split)
    for start in range(0, refs[first_out].shape[0], tile):
        values, at = [], 0
        for parts in split:
            if parts == 1:
                values.append(refs[at][pl.ds(start, tile)])
            elif start == 0:
                values.append(refs[at][...])
            else:
                values.append(refs[at + 1][pl.ds(start - tile, tile)])
            at += parts
        result, other = formula(w, start == 0, *values)
        refs[at][pl.ds(start, tile)] = result
        for (a, b), piece_ref in zip(cuts, refs[at + 1 :]):
            if a <= start < b:
                piece_ref[pl.ds(start - a, tile)] = other


def sums(formula, weights, arrays, cuts, tile):
    rows, heads = arrays[0].shape
    split = [len(array) if isinstance(array, tuple) else 1 for array in arrays]
    flat = jax.tree.leaves(list(arrays))
    held = pl.BlockSpec(memory_space=pltpu.VMEM)
    return pl.pallas_call(
        functools.partial(sums_body, formula, split, cuts, tile),
        in_specs=[pl.BlockSpec(memory_space=pltpu.SMEM)] + [held] * len(flat),
        out_specs=[held] * (1 + len(cuts)),
        out_shape=[jax.ShapeDtypeStruct((rows, heads), jnp.float32)]
        + [jax.ShapeDtypeStruct((b - a, heads), jnp.float32) for a, b in cuts],
        compiler_params=pltpu.CompilerParams(vmem_limit_bytes=SUMS_VMEM),
        cost_estimate=pl.CostEstimate(
            flops=8 * rows * heads, bytes_accessed=28 * rows * heads, transcendentals=0
        ),
    )(weights, *flat)


def near_body(w_ref, own_ref, row_ref, new_ref, old_ref, near_ref, lead_ref):
    near = w_ref[0] * own_ref[...] + w_ref[1] * row_ref[...] + (new_ref[...] - old_ref[...])
    near_ref[...] = near

    @pl.when(pl.program_id(0) == 0)
    def _():
        lead_ref[...] = near


def near_sums(weights, arrays, tile):
    rows, heads = arrays[0].shape
    block = pl.BlockSpec((tile, heads), lambda i: (i, 0))
    return pl.pallas_call(
        near_body,
        grid=(rows // tile,),
        in_specs=[pl.BlockSpec(memory_space=pltpu.SMEM)] + [block] * len(arrays),
        out_specs=[block, pl.BlockSpec((tile, heads), lambda i: (0, 0))],
        out_shape=[
            jax.ShapeDtypeStruct((rows, heads), jnp.float32),
            jax.ShapeDtypeStruct((tile, heads), jnp.float32),
        ],
        compiler_params=pltpu.CompilerParams(
            dimension_semantics=("arbitrary",), vmem_limit_bytes=8 * 2**20
        ),
        cost_estimate=pl.CostEstimate(
            flops=8 * rows * heads, bytes_accessed=24 * rows * heads, transcendentals=0
        ),
        name="near",
    )(weights, *arrays)


def on_device(value_proj, token_pool, target_pool, batch_ids, frozen_out, numerators):
    counts = numerators.astype(jnp.float32)
    is_last = lax.axis_index("col") == lax.axis_size("col") - 1
    mix_weights = counts / jnp.sum(counts)
    weights = jnp.concatenate([mix_weights, is_last.astype(jnp.float32)[None]])
    x0 = value_proj[0, 0]
    width = x0.shape[0]
    lead = width // 8
    middle = width * 5 // 8
    cuts = [(lead, middle), (middle, width), (0, lead)]

    def gradient_at(field, which):
        return local_gradient(
            which, field, token_pool[0, 0], target_pool[0, 0], batch_ids[0, 0], frozen_out
        )

    x0_col = shifted(x0, "col", 1)
    x0_row = shifted(x0, "row", 1)
    g0 = gradient_at(x0, 0)
    g0_rest, g0_lead = lax.optimization_barrier((g0[lead:], g0[:lead]))
    g0_col = (shifted(g0_lead, "col", 1, wraps=False), shifted(g0_rest, "col", 1))
    g0_row = shifted(g0, "row", 1)

    x1, x1_send = sums(step_sum, weights, (x0, x0_row, x0_col, g0), [(0, width)], lead)
    x1_col = shifted(x1_send, "col", 1)
    x1_row = shifted(x1, "row", 1)
    g1 = gradient_at(x1, 1)

    arrays = (g0, g0_row, g0_col, g1, g0)
    t1, *blocks = sums(track_sum, weights, arrays, cuts, lead)
    pieces = [shifted(block, "col", 1) for block in blocks]
    far = last_to_second(mix_weights[2] * mix_weights[2] * g0_lead, "col")
    t1_row = shifted(t1, "row", 1)

    x2, x2_out = sums(plain_step, weights, (x1, x1_row, x1_col, t1), [(0, width)], lead)
    g2 = gradient_at(x2, 2)

    t2, last = near_sums(weights, (t1, t1_row, g2, g1), lead)
    for (start, _), piece in zip(cuts[:-1], pieces):
        t2 = add_piece(t2, piece, start)
    t2 = add_tail(t2, last, pieces[-1], far, cuts[-1][0])
    return (x2_out[None, None], t2[None, None])


def solution(mesh):
    whole = P("row", "col", None, None)
    return jax.shard_map(
        on_device,
        mesh=mesh,
        in_specs=(whole, whole, whole, whole, P(), P()),
        out_specs=(whole, whole),
        check_vma=False,
    )
```
